32 devices in a mesh: rows: 8 (over z, y), cols: 4 (over x, core).
Axes of the slice: x: 2, y: 2, z: 4, core: 2. Of those that a mesh axis runs over, the one named last changes fastest.
Arguments:
- features: bfloat16 [64, 512, 512], P('rows', 'cols'), may hold values from -6 to 6
- dw_weight: float32 [49, 512], replicated, may hold values from -0.875 to 0.875
- norm_gain: float32 [512], replicated, may hold values from 0.1 to 1.9
- w_up: bfloat16 [512, 2048], replicated, may hold values from -0.25 to 0.25
- w_down: bfloat16 [2048, 512], replicated, may hold values from -0.125 to 0.125
- cotangent: bfloat16 [64, 512, 512], P('rows', 'cols'), may hold values from -6 to 6
Outputs:
- grad_input: bfloat16 [64, 512, 512], P('rows', 'cols')
- grad_dw: float32 [49, 512], replicated
- grad_gain: float32 [512], replicated
- grad_up: float32 [512, 2048], replicated
- grad_down: float32 [2048, 512], replicated
The draws below stay inside these ranges and needn't reach their ends.
All inputs are finite; a program needn't handle non-finite values.
Results may differ from the reference program's by a relative error of at most 0.019.
Values may be sent and summed in bfloat16 or wider, within the bound.
A program may use at most 128 MiB of HBM per device.

```python
import jax
import jax.numpy as jnp
from jax import lax

C = 512
FF = 2048
KK = 49
H = 64
W = 512


def shard_levels(stream_key, shape, split, smallest, largest):
    level, own = 1.0, jax.random.fold_in(stream_key, 6)
    for dim, parts in split:
        steps = jnp.exp(jax.random.uniform(jax.random.fold_in(own, dim), (parts,), jnp.float32, smallest / len(split), largest / len(split)))
        level = level * jnp.repeat(steps, shape[dim] // parts).reshape([-1 if axis == dim else 1 for axis in range(len(shape))])
    return level


def normal_values(rng, dims, scale, bound, split=(), kind=jnp.bfloat16):
    values = jax.random.normal(rng, dims, jnp.float32) * scale
    if len(split) > 0:
        values = shard_levels(rng, dims, split, -0.22, 0.18) * values
    return jnp.clip(values, min=-bound, max=bound).astype(kind)


def setup_inputs(seed: int = 0) -> dict:
    keys = jax.random.split(jax.random.key(seed), 7)
    features = normal_values(keys[0], (H, W, C), 1.0, 6.0, ((0, 8), (1, 4)))
    dw_weight = normal_values(keys[1], (KK, C), KK ** -0.5, 0.875, (), jnp.float32)
    norm_gain = jnp.clip(1.0 + 0.18 * jax.random.normal(keys[2], (C,), jnp.float32), 0.1, 1.9)
    w_up = normal_values(keys[3], (C, FF), C ** -0.5, 0.25)
    w_down = normal_values(keys[4], (FF, C), FF ** -0.5, 0.125)
    cotangent = normal_values(keys[5], (H, W, C), 1.0, 6.0, ((0, 8), (1, 4)))
    return {"features": features, "dw_weight": dw_weight, "norm_gain": norm_gain, "w_up": w_up, "w_down": w_down, "cotangent": cotangent}


eps = 1e-06

def depthwise(padded, weight, rows, cols):
    total = jnp.zeros((rows, cols, padded.shape[2]), jnp.float32)
    for tap_i in range(7):
        for tap_j in range(7):
            total = total + padded[tap_i:tap_i + rows, tap_j:tap_j + cols] * weight[7 * tap_i + tap_j]
    return total

def pointwise(conv, gain, w_up, w_down, grad_out):
    mean = lax.optimization_barrier(jnp.mean(conv, axis=-1, keepdims=True))
    centred = conv - mean
    inv = lax.rsqrt(lax.optimization_barrier(jnp.mean(centred * centred, axis=-1, keepdims=True)) + eps)
    normed = centred * inv
    scaled = (normed * gain).astype(jnp.bfloat16)
    hidden = jnp.dot(scaled, w_up, preferred_element_type=jnp.float32)
    act = (0.5 * hidden * (1.0 + lax.erf(hidden * 0.7071067811865476))).astype(jnp.bfloat16)
    grad_down = lax.dot_general(act, grad_out, (((0,), (0,)), ((), ())), preferred_element_type=jnp.float32)
    grad_act = lax.dot_general(grad_out, w_down, (((1,), (1,)), ((), ())), preferred_element_type=jnp.float32)
    slope = 0.5 * (1.0 + lax.erf(hidden * 0.7071067811865476)) + hidden * jnp.exp(-0.5 * hidden * hidden) * 0.3989422804014327
    grad_hidden = (grad_act * slope).astype(jnp.bfloat16)
    grad_up = lax.dot_general(scaled, grad_hidden, (((0,), (0,)), ((), ())), preferred_element_type=jnp.float32)
    grad_scaled = lax.dot_general(grad_hidden, w_up, (((1,), (1,)), ((), ())), preferred_element_type=jnp.float32)
    grad_gain = lax.optimization_barrier(jnp.sum(grad_scaled * normed, axis=0))
    g_norm = grad_scaled * gain
    grad_conv = inv * (g_norm - lax.optimization_barrier(jnp.mean(g_norm, axis=-1, keepdims=True)) - normed * lax.optimization_barrier(jnp.mean(g_norm * normed, axis=-1, keepdims=True)))
    return (grad_conv.astype(jnp.bfloat16), grad_up, grad_down, grad_gain)

def reference(features, dw_weight, norm_gain, w_up, w_down, cotangent):
    padded = jnp.pad(features.astype(jnp.float32), ((3, 3), (3, 3), (0, 0)))
    conv = depthwise(padded, dw_weight, H, W)
    blocks = H // 8
    conv_blocks = conv.reshape(blocks, 8 * W, C)
    grad_blocks = cotangent.reshape(blocks, 8 * W, C)

    def step(carry, pair):
        grad_conv, grad_up, grad_down, grad_gain = pointwise(pair[0], norm_gain, w_up, w_down, pair[1])
        return ((carry[0] + grad_up, carry[1] + grad_down, carry[2] + grad_gain), grad_conv)
    start = (jnp.zeros((C, FF), jnp.float32), jnp.zeros((FF, C), jnp.float32), jnp.zeros((C,), jnp.float32))
    sums, grad_conv = lax.scan(step, start, (conv_blocks, grad_blocks))
    grad_conv = grad_conv.reshape(H, W, C)
    grad_f = grad_conv.astype(jnp.float32)
    taps = []
    for tap_i in range(7):
        for tap_j in range(7):
            taps.append(lax.optimization_barrier(jnp.sum(padded[tap_i:tap_i + H, tap_j:tap_j + W] * grad_f, axis=(0, 1))))
    grad_dw = jnp.stack(taps)
    grad_pad = jnp.pad(grad_f, ((3, 3), (3, 3), (0, 0)))
    total = cotangent.astype(jnp.float32)
    for tap_i in range(7):
        for tap_j in range(7):
            total = total + grad_pad[6 - tap_i:6 - tap_i + H, 6 - tap_j:6 - tap_j + W] * dw_weight[7 * tap_i + tap_j]
    return (total.astype(jnp.bfloat16), grad_dw, sums[2], sums[0], sums[1])
```

```python
import jax
import jax.numpy as jnp
from jax import lax
from jax.experimental import pallas as pl
from jax.experimental.pallas import tpu as pltpu
from jax.sharding import PartitionSpec as P

eps = 1e-06

LANES = 128
STEP = 16


def conv_kernel(has_base, *refs):
    if has_base:
        x_ref, w_ref, base_ref, out_ref, wide, taps = refs
    else:
        x_ref, w_ref, out_ref, wide, taps = refs
    rows, cols, _ = out_ref.shape
    wide[...] = x_ref[...].astype(jnp.float32)
    for k in range(49):
        taps[k] = jnp.broadcast_to(w_ref[k : k + 1, :], (8, LANES))

    def step(c, carry):
        at = pl.multiple_of(c * STEP, STEP)
        if has_base:
            acc = [base_ref[r, pl.ds(at, STEP), :].astype(jnp.float32) for r in range(rows)]
        else:
            acc = [None] * rows
        for j in range(7):
            weights = [jnp.concatenate([taps[7 * i + j]] * 2, axis=0) for i in range(7)]
            for r in range(rows + 6):
                x = wide[r, pl.ds(at + j, STEP), :]
                for i in range(7):
                    if 0 <= r - i < rows:
                        term = x * weights[i]
                        acc[r - i] = term if acc[r - i] is None else acc[r - i] + term
        for r in range(rows):
            out_ref[r, pl.ds(at, STEP), :] = acc[r].astype(out_ref.dtype)
        return carry

    lax.fori_loop(0, cols // STEP, step, 0)


def dw_kernel(x_ref, g_ref, out_ref, wide, sums):
    rows, cols, _ = g_ref.shape
    wide[...] = x_ref[...].astype(jnp.float32)
    sums[...] = jnp.zeros_like(sums)

    def step(c, carry):
        at = pl.multiple_of(c * STEP, STEP)
        grad = [g_ref[r, pl.ds(at, STEP), :].astype(jnp.float32) for r in range(rows)]
        for j in range(7):
            acc = [sums[7 * i + j] for i in range(7)]
            for r in range(rows + 6):
                x = wide[r, pl.ds(at + j, STEP), :]
                for i in range(7):
                    if 0 <= r - i < rows:
                        term = x * grad[r - i]
                        acc[i] = acc[i] + (term[:8] + term[8:])
            for i in range(7):
                sums[7 * i + j] = acc[i]
        return carry

    lax.fori_loop(0, cols // STEP, step, 0)
    for k in range(49):
        out_ref[k : k + 1, :] = jnp.sum(sums[k], axis=0, keepdims=True)


def block3(shape):
    return pl.BlockSpec((shape[0], shape[1], LANES), lambda c: (0, 0, c))


def depthwise(wide, weight, rows, cols, base=None):
    chans = wide.shape[2]
    args = [wide, weight] + ([] if base is None else [base])
    specs = [block3(wide.shape), pl.BlockSpec((49, LANES), lambda c: (0, c))]
    if base is not None:
        specs.append(block3(base.shape))
    kind = jnp.float32 if base is None else jnp.bfloat16
    return pl.pallas_call(
        lambda *refs: conv_kernel(base is not None, *refs),
        grid=(chans // LANES,),
        in_specs=specs,
        out_specs=block3((rows, cols)),
        out_shape=jax.ShapeDtypeStruct((rows, cols, chans), kind),
        scratch_shapes=[
            pltpu.VMEM((wide.shape[0], wide.shape[1], LANES), jnp.float32),
            pltpu.VMEM((49, 8, LANES), jnp.float32),
        ],
        cost_estimate=pl.CostEstimate(
            flops=100 * rows * cols * chans, bytes_accessed=4 * rows * cols * chans, transcendentals=0
        ),
        name="conv",
    )(*args)


def depthwise_grad(wide, grad):
    rows, cols, chans = grad.shape
    return pl.pallas_call(
        dw_kernel,
        grid=(chans // LANES,),
        in_specs=[block3(wide.shape), block3(grad.shape)],
        out_specs=pl.BlockSpec((49, LANES), lambda c: (0, c)),
        out_shape=jax.ShapeDtypeStruct((49, chans), jnp.float32),
        scratch_shapes=[
            pltpu.VMEM((wide.shape[0], wide.shape[1], LANES), jnp.float32),
            pltpu.VMEM((49, 8, LANES), jnp.float32),
        ],
        cost_estimate=pl.CostEstimate(
            flops=100 * rows * cols * chans, bytes_accessed=4 * rows * cols * chans, transcendentals=0
        ),
        name="dw",
    )(wide, grad)


def padded_2(block, sides, width):
    for axis, dim in sides:
        count = lax.axis_size(axis)
        forward = [(i, i + 1) for i in range(count - 1)]
        backward = [(target, source) for source, target in forward]
        low = lax.ppermute(
            lax.slice_in_dim(block, block.shape[dim] - width, None, axis=dim), axis, forward
        )
        high = lax.ppermute(lax.slice_in_dim(block, 0, width, axis=dim), axis, backward)
        block = jnp.concatenate([low, block, high], axis=dim)
    return block


def pointwise(conv, gain, w_up, w_down, grad_out):
    mean = jnp.mean(conv, axis=-1, keepdims=True)
    centred = conv - mean
    inv = lax.rsqrt(jnp.mean(centred * centred, axis=-1, keepdims=True) + eps)
    normed = centred * inv
    scaled = (normed * gain).astype(jnp.bfloat16)
    hidden = jnp.dot(scaled, w_up, preferred_element_type=jnp.float32)
    act = (0.5 * hidden * (1.0 + lax.erf(hidden * 0.7071067811865476))).astype(jnp.bfloat16)
    grad_down = lax.dot_general(
        act, grad_out, (((0,), (0,)), ((), ())), preferred_element_type=jnp.float32
    )
    grad_act = lax.dot_general(
        grad_out, w_down, (((1,), (1,)), ((), ())), preferred_element_type=jnp.float32
    )
    slope = (
        0.5 * (1.0 + lax.erf(hidden * 0.7071067811865476))
        + hidden * jnp.exp(-0.5 * hidden * hidden) * 0.3989422804014327
    )
    grad_hidden = (grad_act * slope).astype(jnp.bfloat16)
    grad_up = lax.dot_general(
        scaled, grad_hidden, (((0,), (0,)), ((), ())), preferred_element_type=jnp.float32
    )
    grad_scaled = lax.dot_general(
        grad_hidden, w_up, (((1,), (1,)), ((), ())), preferred_element_type=jnp.float32
    )
    grad_gain = jnp.sum(grad_scaled * normed, axis=0)
    g_norm = grad_scaled * gain
    grad_conv = inv * (
        g_norm
        - jnp.mean(g_norm, axis=-1, keepdims=True)
        - normed * jnp.mean(g_norm * normed, axis=-1, keepdims=True)
    )
    return (grad_conv.astype(jnp.bfloat16), grad_up, grad_down, grad_gain)


def on_device(features, dw_weight, norm_gain, w_up, w_down, cotangent):
    rows, cols, chans = features.shape
    extra = -(cols + 6) % STEP

    def widened(block):
        return jnp.pad(
            padded_2(block, (("rows", 0), ("cols", 1)), 3), ((0, 0), (0, extra), (0, 0))
        )

    padded = widened(features)
    conv = depthwise(padded, dw_weight, rows, cols)
    grad_flat, grad_up, grad_down, grad_gain = pointwise(
        conv.reshape(rows * cols, chans),
        norm_gain,
        w_up,
        w_down,
        cotangent.reshape(rows * cols, chans),
    )
    grad_down = lax.psum(grad_down.astype(jnp.bfloat16), ("rows", "cols"))
    grad_conv = grad_flat.reshape(rows, cols, chans)
    grad_dw = depthwise_grad(padded, grad_conv)
    small = jnp.concatenate([grad_dw, grad_gain[None]], axis=0)
    grad_up, small = lax.psum(
        (grad_up.astype(jnp.bfloat16), small.astype(jnp.bfloat16)), ("rows", "cols")
    )
    grad_input = depthwise(widened(grad_conv), dw_weight[::-1], rows, cols, cotangent)
    small = small.astype(jnp.float32)
    return (
        grad_input,
        small[:49],
        small[49],
        grad_up.astype(jnp.float32),
        grad_down.astype(jnp.float32),
    )


def solution(mesh):
    return jax.shard_map(
        on_device,
        mesh=mesh,
        in_specs=(P("rows", "cols", None), P(), P(), P(), P(), P("rows", "cols", None)),
        out_specs=(P("rows", "cols", None), P(), P(), P(), P()),
        check_vma=False,
    )
```
